32 devices in a mesh: sector: 2 (over y), term: 16 (over z, x, core).
Axes of the slice: x: 2, y: 2, z: 4, core: 2. Of those that a mesh axis runs over, the one named last changes fastest.
Arguments:
- wave_in: bfloat16 [16, 1024, 256], P('sector'), may hold values from -6 to 6
- left_env: bfloat16 [16, 192, 1024, 256], P('sector', 'term'), may hold values from -0.1875 to 0.1875
- right_env: bfloat16 [16, 192, 256, 64], P('sector', 'term'), may hold values from -0.375 to 0.375
- shift_map: int32 [48, 16], replicated, may hold values from 0 to 15
- live_rows: int32 [16], replicated, may hold values from 512 to 1024
Outputs:
- isometry: bfloat16 [16, 1024, 256], P('sector', 'term')
- env_next: bfloat16 [16, 192, 256, 64], P('sector', 'term')
The draws below stay inside these ranges and needn't reach their ends.
All inputs are finite; a program needn't handle non-finite values.
Results may differ from the reference program's by a relative error of at most 0.014.
Values may be sent and summed in bfloat16 or wider, within the bound.
No kernel may reach another device: no remote copies, remote signals or barrier semaphores. Data moves between devices by JAX's collectives and lax.ppermute only.
A program may use at most 192 MiB of HBM per device.

```python
import math
import jax
import jax.numpy as jnp
from jax import lax

S = 16
TERMS = 48
LEFT_ROWS = 1024
DR = 256
RSL = 4
STEPS = 8
PAIRS = 192
PAIR_DEV = 12
DLR = 256
DRR = 64


def place_ends(values, stream_key, smallest, largest):
    place = [jax.random.randint(jax.random.fold_in(stream_key, axis), (), 0, length) for axis, length in enumerate(values.shape)]
    main_axis = values.shape.index(max(values.shape))
    next_to = place[:main_axis] + [(place[main_axis] + 1) % values.shape[main_axis]] + place[main_axis + 1:]
    return values.at[tuple(place)].set(smallest).at[tuple(next_to)].set(largest)


def block_levels(rng, shape, split, low, largest):
    level = 1.0
    for dim, parts in split:
        steps = jax.random.uniform(jax.random.fold_in(jax.random.fold_in(rng, 6), dim), (parts,), jnp.float32, low / len(split), largest / len(split))
        level = level * jnp.repeat(jnp.exp(steps), shape[dim] // parts).reshape((-1,) + (1,) * (len(shape) - 1 - dim))
    return level


def scatter_about(key, shape, spread, bound, split=(), held_as=jnp.bfloat16):
    entries = spread * jax.random.normal(key, shape, jnp.float32)
    if split:
        entries = entries * block_levels(key, shape, split, -0.22, 0.18)
    return jnp.clip(entries, -bound, bound).astype(held_as)


def setup_inputs(seed: int = 0) -> dict:
    streams_of = jax.random.split(jax.random.key(seed), 6)
    return {
        "wave_in": scatter_about(streams_of[0], (S, LEFT_ROWS, DR), 1.0, 6.0, ((0, 2),)),
        "left_env": scatter_about(streams_of[1], (S, PAIRS, LEFT_ROWS, DLR), LEFT_ROWS ** -0.5, 0.1875, ((0, 2), (1, 16))),
        "right_env": scatter_about(streams_of[2], (S, PAIRS, DR, DRR), DR ** -0.5, 0.375, ((0, 2), (1, 16))),
        "shift_map": place_ends(jax.random.randint(streams_of[3], (TERMS, S), 0, S), jax.random.fold_in(streams_of[3], 1), 0, S - 1).astype(jnp.int32),
        "live_rows": place_ends(jax.random.randint(streams_of[4], (S,), LEFT_ROWS // 2, LEFT_ROWS + 1), jax.random.fold_in(streams_of[4], 1), LEFT_ROWS // 2, LEFT_ROWS).astype(jnp.int32),
    }


step_size = 0.15
epsilon = 1e-06
highest = lax.Precision.HIGHEST

def full_blocks(stacked, per_device):
    width_rows = stacked.shape[1]
    width_cols = stacked.shape[2]
    blocks = stacked.reshape(TERMS // per_device, RSL, per_device, width_rows, width_cols)
    blocks = jnp.transpose(blocks, (0, 2, 3, 1, 4))
    return blocks.reshape(TERMS, width_rows, RSL * width_cols)

def pair_layout(matrices, per_device):
    width_rows = matrices.shape[1]
    width_cols = matrices.shape[2] // RSL
    blocks = matrices.reshape(TERMS // per_device, per_device, width_rows, RSL, width_cols)
    blocks = jnp.transpose(blocks, (0, 3, 1, 2, 4))
    return blocks.reshape(TERMS * RSL, width_rows, width_cols)

def reference(wave_in, left_env, right_env, shift_map, live_rows):
    identity = jnp.eye(DR, dtype=jnp.float32)
    row_ids = jnp.arange(LEFT_ROWS, dtype=jnp.int32)

    def update(sector):
        left_complete = full_blocks(left_env[sector], PAIR_DEV).astype(jnp.float32)
        right_complete = full_blocks(right_env[sector], PAIR_DEV).astype(jnp.float32)
        sources = shift_map[:, sector]
        selected_block = wave_in[sources].astype(jnp.float32)
        operator_applied = jnp.einsum('zgo,zoy->zgy', selected_block, right_complete).astype(jnp.bfloat16)
        sigma_block_sum = jnp.einsum('hwm,hmx->wx', left_complete, operator_applied.astype(jnp.float32))
        live_mask = row_ids[:, None] < live_rows[sector]
        updated = jnp.where(live_mask, wave_in[sector].astype(jnp.float32) - step_size * sigma_block_sum, 0.0)
        gram_sum = jnp.dot(updated.T, updated, precision=highest)
        trace_sum = jnp.trace(gram_sum) + epsilon
        root_part = gram_sum / trace_sum
        inverse_part = identity
        for ns_step in range(STEPS):
            ns_factor = 1.5 * identity - 0.5 * jnp.dot(inverse_part, root_part, precision=highest)
            root_part = jnp.dot(root_part, ns_factor, precision=highest)
            inverse_part = jnp.dot(ns_factor, inverse_part, precision=highest)
        result = jnp.dot(updated, inverse_part, precision=highest) * jnp.sqrt(LEFT_ROWS / trace_sum)
        return result.astype(jnp.bfloat16)
    isometry = lax.map(update, jnp.arange(S, dtype=jnp.int32))

    def renorm(sector):
        left_complete = full_blocks(left_env[sector], PAIR_DEV).astype(jnp.float32)
        projected_wave = jnp.einsum('ia,tib->tab', isometry[sector].astype(jnp.float32), left_complete).astype(jnp.bfloat16)
        selected_block = isometry[shift_map[:, sector]].astype(jnp.float32)
        environment_block = jnp.einsum('zgo,zoy->zgy', projected_wave.astype(jnp.float32), selected_block) / math.sqrt(LEFT_ROWS)
        return pair_layout(environment_block.astype(jnp.bfloat16), PAIR_DEV)
    env_next = lax.map(renorm, jnp.arange(S, dtype=jnp.int32))
    return (isometry, env_next)
```

```python
import functools
import math

import jax
import jax.numpy as jnp
from jax import lax
from jax.experimental import pallas as pl
from jax.experimental.pallas import tpu as pltpu
from jax.sharding import PartitionSpec as P


STEPS = 8
step_size = 0.15
epsilon = 1e-06
f32 = jnp.float32
bf16 = jnp.bfloat16
NT = (((1,), (1,)), ((), ()))


def from_partner(block, axis, bit):
    count = lax.axis_size(axis)
    route = []
    for low in range(count):
        high = low | 1 << bit
        if high != low and high < count:
            route += [(low, high), (high, low)]
    return lax.ppermute(block, axis, route)


def divisor(count, most):
    return max(d for d in range(1, most + 1) if count % d == 0)


def aligned(index, size):
    return pl.ds(pl.multiple_of(index * size, size), size)


def dot(a, b):
    return jnp.dot(a, b, preferred_element_type=f32)


def dot_nt(a, b):
    return lax.dot_general(a, b, NT, preferred_element_type=f32)


def sigma_kernel(slices, terms, meta, idx, *refs):
    w_refs, refs = refs[:terms], refs[terms:]
    right_refs, refs = refs[:slices], refs[slices:]
    left_refs, (keep_ref, send_ref, acc, right, applied) = refs[:terms], refs[terms:]
    rows, part = left_refs[0].shape[2:]
    far, group, groups = pl.program_id(0), pl.program_id(2), pl.num_programs(2)
    me = meta[0]
    own_slice = jnp.bitwise_and(me, slices - 1)
    share = right_refs[0].shape[2]
    for j in range(terms):
        for k, ref in enumerate(right_refs):
            right[j, aligned(jnp.bitwise_xor(own_slice, k), share), :] = ref[0, j]
        applied[j * part:(j + 1) * part, :] = dot_nt(w_refs[j][0], right[j]).astype(bf16)
    tile = min(rows, 512)

    def rows_step(m, carry):
        at = aligned(m, tile)
        left = jnp.concatenate([ref[0, 0, at, :] for ref in left_refs], axis=1)
        value = dot(left, applied[...])

        @pl.when(group == 0)
        def _():
            acc[at, :] = value

        @pl.when(group > 0)
        def _():
            acc[at, :] += value

        return carry

    lax.fori_loop(0, rows // tile, rows_step, 0)
    half = rows // 2
    upper = jnp.bitwise_and(lax.div(me, slices), 1)

    def emit(out):
        for q in range(2):
            out[q, 0] = acc[aligned(jnp.bitwise_xor(upper, q), half), :].astype(bf16)

    @pl.when((group == groups - 1) & (far == 0))
    def _():
        emit(keep_ref)

    @pl.when((group == groups - 1) & (far == 1))
    def _():
        emit(send_ref)


def sigma_call(meta, idx, every_rows, rights, firsts, left_env, first, count):
    _, pair_dev, rows, part = left_env.shape
    share, width = rights[0].shape[2:]
    terms = divisor(pair_dev, 3)
    pairs = count // 2

    def at(h, i, m):
        return jnp.bitwise_xor(h, jnp.bitwise_and(m[0], 1)) * pairs + i

    def source_spec(j):
        return pl.BlockSpec(
            (1,) + every_rows.shape[1:], lambda h, i, g, m, x: (x[at(h, i, m), g * terms + j], 0, 0)
        )

    def right_spec(start):
        return pl.BlockSpec(
            (1, terms, share, width), lambda h, i, g, m, x: (at(h, i, m) + start, g, 0, 0)
        )

    def left_spec(j):
        return pl.BlockSpec(
            (1, 1, rows, part), lambda h, i, g, m, x: (at(h, i, m) + first, g * terms + j, 0, 0)
        )

    out = jax.ShapeDtypeStruct((2, pairs, rows // 2, width), bf16)
    block = (2, 1, rows // 2, width)
    return pl.pallas_call(
        functools.partial(sigma_kernel, len(rights), terms),
        out_shape=(out, out),
        grid_spec=pltpu.PrefetchScalarGridSpec(
            num_scalar_prefetch=2,
            grid=(2, pairs, pair_dev // terms),
            in_specs=[source_spec(j) for j in range(terms)]
            + [right_spec(start) for start in firsts]
            + [left_spec(j) for j in range(terms)],
            out_specs=(
                pl.BlockSpec(block, lambda h, i, g, m, x: (0, jnp.where(h == 0, i, pairs - 1), 0, 0)),
                pl.BlockSpec(block, lambda h, i, g, m, x: (0, jnp.where(h == 0, 0, i), 0, 0)),
            ),
            scratch_shapes=[
                pltpu.VMEM((rows, width), f32),
                pltpu.VMEM((terms, width, width), bf16),
                pltpu.VMEM((terms * part, width), bf16),
            ],
        ),
        cost_estimate=pl.CostEstimate(
            flops=2 * count * pair_dev * width * part * (rows + width),
            bytes_accessed=2 * count * pair_dev * rows * part,
            transcendentals=0,
        ),
        compiler_params=pltpu.CompilerParams(
            dimension_semantics=("arbitrary",) * 3, vmem_limit_bytes=40 << 20
        ),
        name="sigma",
    )(meta, idx, *[every_rows] * terms, *rights, *[left_env] * terms)


def split(a):
    high = a.astype(bf16)
    return high, (a - high.astype(f32)).astype(bf16)


def mm3(a, b):
    (ah, al), (bh, bl) = a, b
    return dot(jnp.concatenate([ah, ah, al], axis=1), jnp.concatenate([bh, bl, bh], axis=0))


def update_kernel(slices, each, meta, limits, own_ref, far_ref, wave_ref, iso_ref, rows_ref, up):
    me = meta[0]
    step = pl.program_id(0)
    half, width = own_ref.shape[1:]
    rows = wave_ref.shape[1]
    block = rows_ref.shape[2]
    ri = lax.broadcasted_iota(jnp.int32, (width, width), 0)
    ci = lax.broadcasted_iota(jnp.int32, (width, width), 1)
    eye = jnp.where(ri == ci, 1.0, 0.0).astype(f32)
    upper = jnp.bitwise_and(lax.div(me, slices), 1)
    grams, sizes, ups = [], [], []
    for n in range(each):
        limit = limits[step * each + n]
        for q, ref in enumerate((own_ref, far_ref)):
            at = jnp.bitwise_xor(upper, q)
            wave = wave_ref[n, aligned(at, half), :].astype(f32)
            live = at * half + lax.broadcasted_iota(jnp.int32, (half, width), 0) < limit
            up[n, aligned(at, half), :] = jnp.where(live, wave - step_size * ref[n].astype(f32), 0.0)
        high, low = split(up[n].T)
        cross = dot_nt(high, low)
        gram = dot_nt(high, high) + (cross + cross.T)
        size = jnp.sum(jnp.sum(gram * eye, axis=1, keepdims=True), axis=0, keepdims=True) + epsilon
        ups.append((high, low))
        grams.append(gram)
        sizes.append(size)
    roots = [gram / size for gram, size in zip(grams, sizes)]
    inverses = [None] * each
    for ns_step in range(STEPS):
        if ns_step == 0:
            products = roots
            roots = [split(root) for root in roots]
        else:
            roots = [split(root) for root in roots]
            products = [mm3(inverse, root) for inverse, root in zip(inverses, roots)]
        factors = [split(1.5 * eye - 0.5 * product) for product in products]
        if ns_step < STEPS - 1:
            roots = [mm3(root, factor) for root, factor in zip(roots, factors)]
        if ns_step == 0:
            inverses = factors
        else:
            inverses = [split(mm3(factor, inverse)) for factor, inverse in zip(factors, inverses)]
    for n in range(each):
        scale = jnp.sqrt(rows / sizes[n])
        iso_ref[n] = (mm3(inverses[n], ups[n]) * scale).astype(bf16)
        for q in range(2):
            own = split(up[n, aligned(jnp.bitwise_xor(me, q), block), :])
            rows_ref[q, n] = (mm3(own, inverses[n]) * scale).astype(bf16)


def update_call(meta, limits, own, far, wave_in, first, slices, positions):
    pairs, half, width = own.shape
    rows = wave_in.shape[1]
    each = divisor(pairs, 2)
    piece = pl.BlockSpec((each, half, width), lambda s, m, i: (s, 0, 0))
    return pl.pallas_call(
        functools.partial(update_kernel, slices, each),
        out_shape=(
            jax.ShapeDtypeStruct((pairs, width, rows), bf16),
            jax.ShapeDtypeStruct((2, pairs, rows // positions, width), bf16),
        ),
        grid_spec=pltpu.PrefetchScalarGridSpec(
            num_scalar_prefetch=2,
            grid=(pairs // each,),
            in_specs=[
                piece,
                piece,
                pl.BlockSpec(
                    (each, rows, width),
                    lambda s, m, i: (
                        s + (first + jnp.bitwise_and(m[0], 1) * pairs) // each, 0, 0
                    ),
                ),
            ],
            out_specs=(
                pl.BlockSpec((each, width, rows), lambda s, m, i: (s, 0, 0)),
                pl.BlockSpec((2, each, rows // positions, width), lambda s, m, i: (0, s, 0, 0)),
            ),
            scratch_shapes=[pltpu.VMEM((each, rows, width), f32)],
        ),
        cost_estimate=pl.CostEstimate(
            flops=pairs * (3 * 2 * width**3 * 21 + 6 * 2 * width * width * rows),
            bytes_accessed=pairs * rows * width * 8,
            transcendentals=0,
        ),
        compiler_params=pltpu.CompilerParams(
            dimension_semantics=("arbitrary",), vmem_limit_bytes=40 << 20
        ),
        name="update",
    )(meta, limits, own, far, wave_in)


def renorm_kernel(slices, terms, scale, meta, idx, iso_ref, *refs):
    part_refs, left_refs, (keep_ref, send_ref) = refs[:terms], refs[terms:2 * terms], refs[2 * terms:]
    own_slice = jnp.bitwise_and(meta[0], slices - 1)
    share = keep_ref.shape[3]
    for j in range(terms):
        front = dot(iso_ref[0], left_refs[j][0, 0]).astype(bf16)
        picked = jnp.concatenate(
            [part_refs[j][0, aligned(jnp.bitwise_xor(own_slice, k), share), :] for k in range(slices)],
            axis=0,
        )
        value = (dot_nt(picked, front) * scale).astype(bf16)
        for k in range(slices):
            out = send_ref if k % 2 else keep_ref
            out[k // 2, 0, j] = value[k * share:(k + 1) * share]


def renorm_call(meta, idx, iso, within, parts, left_env, first, slices):
    _, pair_dev, rows, part = left_env.shape
    pairs, width = iso.shape[0] // 2, iso.shape[1]
    share = width // slices
    terms = divisor(pair_dev, 3)

    def part_spec(j):
        return pl.BlockSpec((1,) + parts.shape[1:], lambda g, m, x: (x[g * terms + j], 0, 0))

    def left_spec(j):
        return pl.BlockSpec((1, 1, rows, part), lambda g, m, x: (first, g * terms + j, 0, 0))

    out = jax.ShapeDtypeStruct((slices // 2, 1, pair_dev, share, width), bf16)
    out_spec = pl.BlockSpec((slices // 2, 1, terms, share, width), lambda g, m, x: (0, 0, g, 0, 0))
    return pl.pallas_call(
        functools.partial(renorm_kernel, slices, terms, 1 / math.sqrt(rows)),
        out_shape=(out, out),
        grid_spec=pltpu.PrefetchScalarGridSpec(
            num_scalar_prefetch=2,
            grid=(pair_dev // terms,),
            in_specs=[
                pl.BlockSpec(
                    (1, width, rows),
                    lambda g, m, x: (
                        jnp.bitwise_xor(within // pairs, jnp.bitwise_and(m[0], 1)) * pairs
                        + within % pairs, 0, 0
                    ),
                )
            ]
            + [part_spec(j) for j in range(terms)]
            + [left_spec(j) for j in range(terms)],
            out_specs=(out_spec, out_spec),
        ),
        cost_estimate=pl.CostEstimate(
            flops=2 * pair_dev * width * part * (rows + width),
            bytes_accessed=2 * pair_dev * rows * part,
            transcendentals=0,
        ),
        compiler_params=pltpu.CompilerParams(
            dimension_semantics=("arbitrary",), vmem_limit_bytes=40 << 20
        ),
        name="renorm",
    )(meta, idx, iso, *[parts] * terms, *[left_env] * terms)


def every_sector(block):
    for bit in range((lax.axis_size("sector") - 1).bit_length()):
        block = jnp.concatenate([block, from_partner(block, "sector", bit)], axis=0)
    return block


def add(a, b):
    return (a.astype(f32) + b.astype(f32)).astype(bf16)


def sum_terms(keep, send, slice_bits, all_bits):
    total = add(keep, from_partner(send, "term", 0))
    mine = add(total[0], from_partner(total[1], "term", slice_bits))
    others = list(range(slice_bits + 1, all_bits)) + list(range(1, slice_bits))
    for bit in others:
        mine = add(mine, from_partner(mine, "term", bit))
    return mine, from_partner(mine, "term", slice_bits)


def body(wave_in, left_env, right_env, shift_map, live_rows):
    sec_dev, rows, width = wave_in.shape
    pair_dev = left_env.shape[1]
    slices = rows // left_env.shape[3]
    part = rows // slices
    slice_bits = slices.bit_length() - 1
    positions = lax.axis_size("term")
    all_bits = positions.bit_length() - 1
    sectors = lax.axis_size("sector")
    me = lax.axis_index("term")
    my_sector = lax.axis_index("sector")
    own_slice = me % slices
    core = me % 2
    meta = jnp.reshape(me, (1,)).astype(jnp.int32)
    first_sector = my_sector * sec_dev
    terms_here = lax.dynamic_slice_in_dim(shift_map, (me // slices) * pair_dev, pair_dev, 0)
    sources = lax.dynamic_slice_in_dim(terms_here, first_sector, sec_dev, 1).T
    far_device = (sources // sec_dev) ^ my_sector
    sources = sources % sec_dev
    limits = lax.dynamic_slice_in_dim(live_rows, first_sector, sec_dev, 0)
    right = jnp.swapaxes(right_env, 2, 3)

    size = 2
    pairs = size // 2
    chunks = [(first, size) for first in range(0, sec_dev, size)]
    in_chunk = sources % size
    placed = (sources // size) * size + ((in_chunk // pairs) ^ core) * pairs + in_chunk % pairs
    wave_idx = far_device * sec_dev + sources
    part_idx = far_device * sec_dev + placed

    mine_rows = lax.dynamic_slice_in_dim(wave_in, own_slice * part, part, 1)
    every_rows = every_sector(mine_rows)
    near = from_partner(right, "term", 0)

    isos, own_rows, send_rows = [], [], []
    every_part = jnp.zeros((sectors, sec_dev, width, part), bf16)
    for first, count in chunks:
        blocks = {0: right, 1: near}
        own = lax.slice_in_dim(right, first, first + count, axis=0)
        for bit in range(1, slice_bits):
            known = [own] + [blocks[k] for k in range(2, 1 << bit, 2)]
            for k, block in zip(range(0, 1 << bit, 2), known):
                there = k | 1 << bit
                blocks[there] = from_partner(block, "term", bit)
                blocks[there + 1] = from_partner(blocks[there], "term", 0)
        starts = [first if k < 2 else 0 for k in range(slices)]
        keep, send = sigma_call(
            meta, wave_idx[first:first + count], every_rows, [blocks[k] for k in range(slices)],
            starts, left_env, first, count,
        )
        own, far = sum_terms(keep, send, slice_bits, all_bits)
        mine_limits = lax.dynamic_slice_in_dim(limits, first + core * pairs, pairs, 0)
        iso, iso_rows = update_call(meta, mine_limits, own, far, wave_in, first, slices, positions)
        iso = jnp.concatenate([iso, from_partner(iso, "term", 0)], axis=0)
        isos.append(iso)
        own_rows.append(iso_rows[0])
        send_rows.append(iso_rows[1])
        iso_part = lax.dynamic_slice_in_dim(iso, own_slice * part, part, 2)
        spread = every_sector(iso_part[None])
        every_part = lax.dynamic_update_slice(every_part, spread, (0, first, 0, 0))
    own_rows = jnp.stack(own_rows)
    far_rows = from_partner(jnp.stack(send_rows), "term", 0)
    lower = jnp.where(core == 0, own_rows, far_rows)
    upper = jnp.where(core == 0, far_rows, own_rows)
    wave_out = jnp.stack([lower, upper], axis=1).reshape(sec_dev, rows // positions, width)
    parts = every_part.reshape(sectors * sec_dev, width, part)

    share = width // slices
    env = jnp.zeros((sec_dev, pair_dev, share, width), bf16)
    for first in range(sec_dev):
        keep, send = renorm_call(
            meta, part_idx[first], isos[first // size], first % size, parts, left_env, first, slices
        )
        value = keep.astype(f32) + from_partner(send, "term", 0).astype(f32)
        value = value.reshape((2,) * (slice_bits - 1) + value.shape[1:])
        for bit in reversed(range(1, slice_bits)):
            value = value[0] + from_partner(value[1].astype(bf16), "term", bit).astype(f32)
        env = lax.dynamic_update_slice(env, value.astype(bf16), (first, 0, 0, 0))
    return wave_out, jnp.swapaxes(env, 2, 3)


def solution(mesh):
    in_specs = (
        P("sector", None, None),
        P("sector", "term", None, None),
        P("sector", "term", None, None),
        P(),
        P(),
    )
    out_specs = (P("sector", "term", None), P("sector", "term", None, None))

    return jax.shard_map(body, mesh=mesh, in_specs=in_specs, out_specs=out_specs, check_vma=False)
```

```python
import functools
import math

import jax
import jax.numpy as jnp
from jax import lax
from jax.experimental import pallas as pl
from jax.experimental.pallas import tpu as pltpu
from jax.sharding import PartitionSpec as P


STEPS = 8
step_size = 0.15
epsilon = 1e-06
f32 = jnp.float32
bf16 = jnp.bfloat16
NT = (((1,), (1,)), ((), ()))


def from_partner(block, axis, bit):
    count = lax.axis_size(axis)
    route = []
    for low in range(count):
        high = low | 1 << bit
        if high != low and high < count:
            route += [(low, high), (high, low)]
    return lax.ppermute(block, axis, route)


def divisor(count, most):
    return max(d for d in range(1, most + 1) if count % d == 0)


def aligned(index, size):
    return pl.ds(pl.multiple_of(index * size, size), size)


def dot(a, b):
    return jnp.dot(a, b, preferred_element_type=f32)


def dot_nt(a, b):
    return lax.dot_general(a, b, NT, preferred_element_type=f32)


def sigma_kernel(slices, terms, once, meta, idx, *refs):
    w_refs, refs = refs[:terms], refs[terms:]
    right_refs, refs = refs[:slices], refs[slices:]
    left_refs, (keep_ref, send_ref, acc, right, applied) = refs[:terms], refs[terms:]
    rows, part = left_refs[0].shape[2:]
    far, group, groups = pl.program_id(0), pl.program_id(2), pl.num_programs(2)
    me = meta[0]
    own_slice = jnp.bitwise_and(me, slices - 1)
    share = right_refs[0].shape[2]
    for j in range(terms):
        for k, ref in enumerate(right_refs):
            right[j, aligned(jnp.bitwise_xor(own_slice, k), share), :] = ref[0, j]
        applied[j * part:(j + 1) * part, :] = dot_nt(w_refs[j][0], right[j]).astype(bf16)
    left = jnp.concatenate([ref[0, 0] for ref in left_refs], axis=1)
    value = dot(left, applied[...])
    if once:
        acc[...] = value.astype(bf16)
    else:

        @pl.when(group == 0)
        def _():
            acc[...] = value

        @pl.when(group > 0)
        def _():
            acc[...] += value

    half = rows // 2
    upper = jnp.bitwise_and(lax.div(me, slices), 1)

    def emit(out):
        for q in range(2):
            out[q, 0] = acc[aligned(jnp.bitwise_xor(upper, q), half), :].astype(bf16)

    @pl.when((group == groups - 1) & (far == 0))
    def _():
        emit(keep_ref)

    @pl.when((group == groups - 1) & (far == 1))
    def _():
        emit(send_ref)


def sigma_call(meta, idx, every_rows, rights, firsts, left_env, first, count):
    _, pair_dev, rows, part = left_env.shape
    share, width = rights[0].shape[2:]
    terms = divisor(pair_dev, 12)
    once = terms == pair_dev
    pairs = count // 2

    def at(h, i, m):
        return jnp.bitwise_xor(h, jnp.bitwise_and(m[0], 1)) * pairs + i

    def source_spec(j):
        return pl.BlockSpec(
            (1,) + every_rows.shape[1:], lambda h, i, g, m, x: (x[at(h, i, m), g * terms + j], 0, 0)
        )

    def right_spec(start):
        return pl.BlockSpec(
            (1, terms, share, width), lambda h, i, g, m, x: (at(h, i, m) + start, g, 0, 0)
        )

    def left_spec(j):
        return pl.BlockSpec(
            (1, 1, rows, part), lambda h, i, g, m, x: (at(h, i, m) + first, g * terms + j, 0, 0)
        )

    out = jax.ShapeDtypeStruct((2, pairs, rows // 2, width), bf16)
    block = (2, 1, rows // 2, width)
    return pl.pallas_call(
        functools.partial(sigma_kernel, len(rights), terms, once),
        out_shape=(out, out),
        grid_spec=pltpu.PrefetchScalarGridSpec(
            num_scalar_prefetch=2,
            grid=(2, pairs, pair_dev // terms),
            in_specs=[source_spec(j) for j in range(terms)]
            + [right_spec(start) for start in firsts]
            + [left_spec(j) for j in range(terms)],
            out_specs=(
                pl.BlockSpec(block, lambda h, i, g, m, x: (0, jnp.where(h == 0, i, pairs - 1), 0, 0)),
                pl.BlockSpec(block, lambda h, i, g, m, x: (0, jnp.where(h == 0, 0, i), 0, 0)),
            ),
            scratch_shapes=[
                pltpu.VMEM((rows, width), bf16 if once else f32),
                pltpu.VMEM((terms, width, width), bf16),
                pltpu.VMEM((terms * part, width), bf16),
            ],
        ),
        cost_estimate=pl.CostEstimate(
            flops=2 * count * pair_dev * width * part * (rows + width),
            bytes_accessed=2 * count * pair_dev * rows * part,
            transcendentals=0,
        ),
        compiler_params=pltpu.CompilerParams(
            dimension_semantics=("arbitrary",) * 3, vmem_limit_bytes=48 << 20
        ),
        name="sigma",
    )(meta, idx, *[every_rows] * terms, *rights, *[left_env] * terms)


def split(a):
    high = a.astype(bf16)
    return high, (a - high.astype(f32)).astype(bf16)


def mm3(a, b):
    (ah, al), (bh, bl) = a, b
    return dot(jnp.concatenate([ah, ah, al], axis=1), jnp.concatenate([bh, bl, bh], axis=0))


def update_kernel(slices, each, meta, limits, own_ref, far_ref, wave_ref, iso_ref, rows_ref, up):
    me = meta[0]
    step = pl.program_id(0)
    half, width = own_ref.shape[1:]
    rows = wave_ref.shape[1]
    block = rows_ref.shape[2]
    ri = lax.broadcasted_iota(jnp.int32, (width, width), 0)
    ci = lax.broadcasted_iota(jnp.int32, (width, width), 1)
    eye = jnp.where(ri == ci, 1.0, 0.0).astype(f32)
    upper = jnp.bitwise_and(lax.div(me, slices), 1)
    grams, sizes, ups = [], [], []
    for n in range(each):
        limit = limits[step * each + n]
        for q, ref in enumerate((own_ref, far_ref)):
            at = jnp.bitwise_xor(upper, q)
            wave = wave_ref[n, aligned(at, half), :].astype(f32)
            live = at * half + lax.broadcasted_iota(jnp.int32, (half, width), 0) < limit
            up[n, aligned(at, half), :] = jnp.where(live, wave - step_size * ref[n].astype(f32), 0.0)
        high, low = split(up[n].T)
        cross = dot_nt(high, low)
        gram = dot_nt(high, high) + (cross + cross.T)
        size = jnp.sum(jnp.sum(gram * eye, axis=1, keepdims=True), axis=0, keepdims=True) + epsilon
        ups.append((high, low))
        grams.append(gram)
        sizes.append(size)
    roots = [gram / size for gram, size in zip(grams, sizes)]
    inverses = [None] * each
    for ns_step in range(STEPS):
        if ns_step == 0:
            products = roots
            roots = [split(root) for root in roots]
        else:
            roots = [split(root) for root in roots]
            products = [mm3(inverse, root) for inverse, root in zip(inverses, roots)]
        factors = [split(1.5 * eye - 0.5 * product) for product in products]
        if ns_step < STEPS - 1:
            roots = [mm3(root, factor) for root, factor in zip(roots, factors)]
        if ns_step == 0:
            inverses = factors
        else:
            inverses = [split(mm3(factor, inverse)) for factor, inverse in zip(factors, inverses)]
    for n in range(each):
        scale = jnp.sqrt(rows / sizes[n])
        iso_ref[n] = (mm3(inverses[n], ups[n]) * scale).astype(bf16)
        for q in range(2):
            own = split(up[n, aligned(jnp.bitwise_xor(me, q), block), :])
            rows_ref[q, n] = (mm3(own, inverses[n]) * scale).astype(bf16)


def update_call(meta, limits, own, far, wave_in, first, slices, positions):
    pairs, half, width = own.shape
    rows = wave_in.shape[1]
    each = divisor(pairs, 2)
    piece = pl.BlockSpec((each, half, width), lambda s, m, i: (s, 0, 0))
    return pl.pallas_call(
        functools.partial(update_kernel, slices, each),
        out_shape=(
            jax.ShapeDtypeStruct((pairs, width, rows), bf16),
            jax.ShapeDtypeStruct((2, pairs, rows // positions, width), bf16),
        ),
        grid_spec=pltpu.PrefetchScalarGridSpec(
            num_scalar_prefetch=2,
            grid=(pairs // each,),
            in_specs=[
                piece,
                piece,
                pl.BlockSpec(
                    (each, rows, width),
                    lambda s, m, i: (
                        s + (first + jnp.bitwise_and(m[0], 1) * pairs) // each, 0, 0
                    ),
                ),
            ],
            out_specs=(
                pl.BlockSpec((each, width, rows), lambda s, m, i: (s, 0, 0)),
                pl.BlockSpec((2, each, rows // positions, width), lambda s, m, i: (0, s, 0, 0)),
            ),
            scratch_shapes=[pltpu.VMEM((each, rows, width), f32)],
        ),
        cost_estimate=pl.CostEstimate(
            flops=pairs * (3 * 2 * width**3 * 21 + 6 * 2 * width * width * rows),
            bytes_accessed=pairs * rows * width * 8,
            transcendentals=0,
        ),
        compiler_params=pltpu.CompilerParams(
            dimension_semantics=("arbitrary",), vmem_limit_bytes=40 << 20
        ),
        name="update",
    )(meta, limits, own, far, wave_in)


def renorm_kernel(slices, terms, scale, meta, idx, iso_ref, *refs):
    part_refs, left_refs, (keep_ref, send_ref) = refs[:terms], refs[terms:2 * terms], refs[2 * terms:]
    own_slice = jnp.bitwise_and(meta[0], slices - 1)
    share = keep_ref.shape[3]
    fronts = [dot(iso_ref[0], left_refs[j][0, 0]).astype(bf16) for j in range(terms)]
    for j, front in enumerate(fronts):
        picked = jnp.concatenate(
            [part_refs[j][0, aligned(jnp.bitwise_xor(own_slice, k), share), :] for k in range(slices)],
            axis=0,
        )
        value = (dot_nt(picked, front) * scale).astype(bf16)
        for k in range(slices):
            out = send_ref if k % 2 else keep_ref
            out[k // 2, 0, j] = value[k * share:(k + 1) * share]


def renorm_call(meta, idx, iso, within, parts, left_env, first, slices):
    _, pair_dev, rows, part = left_env.shape
    pairs, width = iso.shape[0] // 2, iso.shape[1]
    share = width // slices
    terms = divisor(pair_dev, 6)

    def part_spec(j):
        return pl.BlockSpec((1,) + parts.shape[1:], lambda g, m, x: (x[g * terms + j], 0, 0))

    def left_spec(j):
        return pl.BlockSpec((1, 1, rows, part), lambda g, m, x: (first, g * terms + j, 0, 0))

    out = jax.ShapeDtypeStruct((slices // 2, 1, pair_dev, share, width), bf16)
    out_spec = pl.BlockSpec((slices // 2, 1, terms, share, width), lambda g, m, x: (0, 0, g, 0, 0))
    return pl.pallas_call(
        functools.partial(renorm_kernel, slices, terms, 1 / math.sqrt(rows)),
        out_shape=(out, out),
        grid_spec=pltpu.PrefetchScalarGridSpec(
            num_scalar_prefetch=2,
            grid=(pair_dev // terms,),
            in_specs=[
                pl.BlockSpec(
                    (1, width, rows),
                    lambda g, m, x: (
                        jnp.bitwise_xor(within // pairs, jnp.bitwise_and(m[0], 1)) * pairs
                        + within % pairs, 0, 0
                    ),
                )
            ]
            + [part_spec(j) for j in range(terms)]
            + [left_spec(j) for j in range(terms)],
            out_specs=(out_spec, out_spec),
        ),
        cost_estimate=pl.CostEstimate(
            flops=2 * pair_dev * width * part * (rows + width),
            bytes_accessed=2 * pair_dev * rows * part,
            transcendentals=0,
        ),
        compiler_params=pltpu.CompilerParams(
            dimension_semantics=("arbitrary",), vmem_limit_bytes=40 << 20
        ),
        name="renorm",
    )(meta, idx, iso, *[parts] * terms, *[left_env] * terms)


def every_sector(block):
    for bit in range((lax.axis_size("sector") - 1).bit_length()):
        block = jnp.concatenate([block, from_partner(block, "sector", bit)], axis=0)
    return block


def add(a, b):
    return (a.astype(f32) + b.astype(f32)).astype(bf16)


def sum_terms(keep, send, slice_bits, all_bits):
    total = add(keep, from_partner(send, "term", 0))
    mine = add(total[0], from_partner(total[1], "term", slice_bits))
    others = list(range(slice_bits + 1, all_bits)) + list(range(1, slice_bits))
    for bit in others:
        mine = add(mine, from_partner(mine, "term", bit))
    return mine, from_partner(mine, "term", slice_bits)


def body(wave_in, left_env, right_env, shift_map, live_rows):
    sec_dev, rows, width = wave_in.shape
    pair_dev = left_env.shape[1]
    slices = rows // left_env.shape[3]
    part = rows // slices
    slice_bits = slices.bit_length() - 1
    positions = lax.axis_size("term")
    all_bits = positions.bit_length() - 1
    sectors = lax.axis_size("sector")
    me = lax.axis_index("term")
    my_sector = lax.axis_index("sector")
    own_slice = me % slices
    core = me % 2
    meta = jnp.reshape(me, (1,)).astype(jnp.int32)
    first_sector = my_sector * sec_dev
    terms_here = lax.dynamic_slice_in_dim(shift_map, (me // slices) * pair_dev, pair_dev, 0)
    sources = lax.dynamic_slice_in_dim(terms_here, first_sector, sec_dev, 1).T
    far_device = (sources // sec_dev) ^ my_sector
    sources = sources % sec_dev
    limits = lax.dynamic_slice_in_dim(live_rows, first_sector, sec_dev, 0)
    right = jnp.swapaxes(right_env, 2, 3)

    size = 2
    pairs = size // 2
    chunks = [(first, size) for first in range(0, sec_dev, size)]
    in_chunk = sources % size
    placed = (sources // size) * size + ((in_chunk // pairs) ^ core) * pairs + in_chunk % pairs
    wave_idx = far_device * sec_dev + sources
    part_idx = far_device * sec_dev + placed

    mine_rows = lax.dynamic_slice_in_dim(wave_in, own_slice * part, part, 1)
    every_rows = every_sector(mine_rows)
    near = from_partner(right, "term", 0)

    isos, own_rows, send_rows = [], [], []
    every_part = jnp.zeros((sectors, sec_dev, width, part), bf16)
    later = right
    for number, (first, count) in enumerate(chunks):
        blocks = {0: right, 1: near}
        own = lax.slice_in_dim(later, first, first + count, axis=0)
        if number == 0:
            own, later = lax.optimization_barrier((own, later))
        for bit in range(1, slice_bits):
            known = [own] + [blocks[k] for k in range(2, 1 << bit, 2)]
            for k, block in zip(range(0, 1 << bit, 2), known):
                there = k | 1 << bit
                blocks[there] = from_partner(block, "term", bit)
                blocks[there + 1] = from_partner(blocks[there], "term", 0)
        starts = [first if k < 2 else 0 for k in range(slices)]
        keep, send = sigma_call(
            meta, wave_idx[first:first + count], every_rows, [blocks[k] for k in range(slices)],
            starts, left_env, first, count,
        )
        own, far = sum_terms(keep, send, slice_bits, all_bits)
        mine_limits = lax.dynamic_slice_in_dim(limits, first + core * pairs, pairs, 0)
        iso, iso_rows = update_call(meta, mine_limits, own, far, wave_in, first, slices, positions)
        iso = jnp.concatenate([iso, from_partner(iso, "term", 0)], axis=0)
        isos.append(iso)
        own_rows.append(iso_rows[0])
        send_rows.append(iso_rows[1])
        iso_part = lax.dynamic_slice_in_dim(iso, own_slice * part, part, 2)
        spread = every_sector(iso_part[None])
        every_part = lax.dynamic_update_slice(every_part, spread, (0, first, 0, 0))
    own_rows = jnp.stack(own_rows)
    far_rows = from_partner(jnp.stack(send_rows), "term", 0)
    lower = jnp.where(core == 0, own_rows, far_rows)
    upper = jnp.where(core == 0, far_rows, own_rows)
    wave_out = jnp.stack([lower, upper], axis=1).reshape(sec_dev, rows // positions, width)
    parts = every_part.reshape(sectors * sec_dev, width, part)

    share = width // slices
    env = jnp.zeros((sec_dev, pair_dev, share, width), bf16)
    for first in range(sec_dev):
        keep, send = renorm_call(
            meta, part_idx[first], isos[first // size], first % size, parts, left_env, first, slices
        )
        value = keep.astype(f32) + from_partner(send, "term", 0).astype(f32)
        value = value.reshape((2,) * (slice_bits - 1) + value.shape[1:])
        for bit in reversed(range(1, slice_bits)):
            value = value[0] + from_partner(value[1].astype(bf16), "term", bit).astype(f32)
        env = lax.dynamic_update_slice(env, value.astype(bf16), (first, 0, 0, 0))
    return wave_out, jnp.swapaxes(env, 2, 3)


def solution(mesh):
    in_specs = (
        P("sector", None, None),
        P("sector", "term", None, None),
        P("sector", "term", None, None),
        P(),
        P(),
    )
    out_specs = (P("sector", "term", None), P("sector", "term", None, None))

    return jax.shard_map(body, mesh=mesh, in_specs=in_specs, out_specs=out_specs, check_vma=False)
```
